32 devices in a mesh: dp: 8 (over z, x), heads: 4 (over y, core).
Axes of the slice: x: 2, y: 2, z: 4, core: 2. Of those that a mesh axis runs over, the one named last changes fastest.
Arguments:
- queries: bfloat16 [8, 2048, 1024], P(None, ('dp', 'heads')), may hold values from -6 to 6
- keys: bfloat16 [8, 2048, 512], P(None, ('dp', 'heads')), may hold values from -6 to 6
- values: bfloat16 [8, 2048, 512], P(None, ('dp', 'heads')), may hold values from -6 to 6
- lengths: int32 [8, 32], replicated, may hold values from 1 to 256, 2048 in all within a row
Outputs:
- attended: bfloat16 [8, 2048, 1024], P(None, ('dp', 'heads'))
- log_norm: float32 [8, 8, 2048], P('heads', None, 'dp')
The draws below stay inside these ranges and needn't reach their ends.
Inputs may be any that keep to these rules, and one draw needn't show every extreme that they name: In each row the 32 lengths sum to 2048, and the longest is exactly 256.
All inputs are finite; a program needn't handle non-finite values.
Results may differ from the reference program's by a relative error of at most 0.0034.
Values may be sent and summed in bfloat16 or wider, within the bound.
A program may use at most 64 MiB of HBM per device.

```python
import math
import jax
import jax.numpy as jnp
import numpy as np
from jax import lax

HEAD_SIZE = 128
PACKED_ROWS = 8
DOCS = 32
VALUE_KEY_HEADS = 4
QUERY_HEADS = 8
ROW_POSITIONS = 2048
MOST = 256


def draw_queries(key, part):
    sampled_values = jax.random.truncated_normal(jax.random.fold_in(key, 11), -6.0, 6.0, (PACKED_ROWS, ROW_POSITIONS, QUERY_HEADS * HEAD_SIZE), jnp.float32)
    return sampled_values.astype(jnp.bfloat16)


def draw_keys(key, part):
    sampled_values = jax.random.truncated_normal(jax.random.fold_in(key, 23), -6.0, 6.0, (PACKED_ROWS, ROW_POSITIONS, VALUE_KEY_HEADS * HEAD_SIZE), jnp.float32)
    return sampled_values.astype(jnp.bfloat16)


def block_levels(stream_key, shape, split, smallest, top_value):
    factor_of = 1.0
    for dim, shards_of in split:
        heights = jax.random.uniform(jax.random.fold_in(jax.random.fold_in(stream_key, 6), dim), (shards_of,), jnp.float32, smallest / len(split), top_value / len(split))
        factor_of = factor_of * jnp.repeat(jnp.exp(heights), shape[dim] // shards_of).reshape((-1,) + (1,) * (len(shape) - 1 - dim))
    return factor_of


def length_profile(count, total, most, lean):
    weights = [(1 << 20) // math.isqrt(standing ** lean) + 1 for standing in range(2, count + 1)]
    rest, given = total - most - (count - 1), [1] * (count - 1)
    while rest > 0:
        candidates = [i for i in range(count - 1) if given[i] < most]
        pool, remaining = sum([weights[i] for i in candidates]), rest
        for i in candidates:
            more = min(most - given[i], max(1, remaining * weights[i] // pool), rest)
            given[i] = given[i] + more
            rest = rest - more
    return np.array([most] + given)


def uneven_parts(own_key, number_of, total, reach, skew):
    if number_of == 2:
        one = jax.random.randint(own_key, (), max(1, total - reach), min(reach, total - 1) + 1)
        return jnp.stack([one, total - one])
    sizes = jnp.asarray(length_profile(number_of, total, reach, skew), jnp.int32)
    pairs = (number_of - 1) // 2
    giver, taker = sizes[1:1 + 2 * pairs:2], sizes[2:2 + 2 * pairs:2]
    room = jnp.minimum(giver - 1, reach - taker)
    moved = jax.random.randint(jax.random.fold_in(own_key, 1), (pairs,), 0, 1 << 20) % (room + 1)
    sizes = sizes.at[1:1 + 2 * pairs:2].set(giver - moved).at[2:2 + 2 * pairs:2].set(taker + moved)
    return sizes[jax.random.permutation(jax.random.fold_in(own_key, 2), number_of)]


def normal_values(stream_key, extent, width, bound, split=(), kind=jnp.bfloat16):
    loudness = block_levels(stream_key, extent, split, -0.22, 0.18) if split else 1.0
    array = jax.random.normal(stream_key, extent, jnp.float32) * width * loudness
    return jnp.minimum(jnp.maximum(array, -bound), bound).astype(kind)


def setup_inputs(seed: int = 0) -> dict:
    streams_of = jax.random.split(jax.random.key(seed), 5)
    queries = draw_queries(jax.random.fold_in(streams_of[4], 71), 0)
    keys = draw_keys(jax.random.fold_in(streams_of[4], 71), 0)
    values = normal_values(streams_of[2], (PACKED_ROWS, ROW_POSITIONS, VALUE_KEY_HEADS * HEAD_SIZE), 1.0, 6.0, ((1, 32),))
    lengths = jax.vmap(lambda own: uneven_parts(own, DOCS, ROW_POSITIONS, MOST, 2))(jax.random.split(streams_of[3], PACKED_ROWS)).reshape((PACKED_ROWS, DOCS)).astype(jnp.int32)
    return {"queries": queries, "keys": keys, "values": values, "lengths": lengths}


def reference(queries, keys, values, lengths):
    row_count, seq_len, q_width = queries.shape
    heads_q = q_width // HEAD_SIZE
    heads_kv = keys.shape[2] // HEAD_SIZE
    per_group = heads_q // heads_kv
    query_block = min(512, seq_len)
    key_span = min(seq_len, query_block + MOST)
    block_count = seq_len // query_block
    doc_ends = jnp.cumsum(lengths, axis=1).astype(jnp.int32)
    positions = jnp.arange(seq_len, dtype=jnp.int32)
    doc_ids = jnp.sum((doc_ends[:, None, :] <= positions[None, :, None]).astype(jnp.int32), axis=-1)

    def attend_block(flat_index):
        row_index = (flat_index // block_count).astype(jnp.int32)
        query_first = ((flat_index % block_count) * query_block).astype(jnp.int32)
        key_first = jnp.clip(query_first - MOST, 0, seq_len - key_span).astype(jnp.int32)
        zero = jnp.zeros((), jnp.int32)
        query_rows = lax.dynamic_slice(queries, (row_index, query_first, zero), (1, query_block, q_width))[0]
        key_rows = lax.dynamic_slice(keys, (row_index, key_first, zero), (1, key_span, heads_kv * HEAD_SIZE))[0]
        value_rows = lax.dynamic_slice(values, (row_index, key_first, zero), (1, key_span, heads_kv * HEAD_SIZE))[0]
        query_heads = query_rows.reshape(query_block, heads_q, HEAD_SIZE).astype(jnp.float32)
        key_heads = jnp.repeat(key_rows.reshape(key_span, heads_kv, HEAD_SIZE), per_group, axis=1).astype(jnp.float32)
        value_heads = jnp.repeat(value_rows.reshape(key_span, heads_kv, HEAD_SIZE), per_group, axis=1).astype(jnp.float32)
        row_docs = lax.dynamic_slice(doc_ids, (row_index, zero), (1, seq_len))[0]
        query_pos = query_first + jnp.arange(query_block, dtype=jnp.int32)
        key_pos = key_first + jnp.arange(key_span, dtype=jnp.int32)
        query_doc = lax.dynamic_slice_in_dim(row_docs, query_first, query_block, 0)
        key_doc = lax.dynamic_slice_in_dim(row_docs, key_first, key_span, 0)
        visible = (query_doc[:, None] == key_doc[None, :]) & (key_pos[None, :] <= query_pos[:, None])
        scores = jnp.einsum("qhd,khd->hqk", query_heads, key_heads) * (HEAD_SIZE ** -0.5)
        masked = jnp.where(visible[None], scores, -jnp.inf)
        row_max = jnp.max(masked, axis=-1)
        weights = jnp.where(visible[None], jnp.exp(masked - row_max[..., None]), jnp.float32(0.0))
        row_sum = jnp.sum(weights, axis=-1)
        rounded = lax.optimization_barrier(weights.astype(jnp.bfloat16)).astype(jnp.float32)
        summed = jnp.einsum("hqk,khd->qhd", rounded, value_heads)
        result = (summed / jnp.transpose(row_sum)[:, :, None]).astype(jnp.bfloat16)
        log_norm = row_max + jnp.log(row_sum)
        return result.reshape(query_block, q_width), log_norm

    outputs, norms = lax.map(attend_block, jnp.arange(row_count * block_count, dtype=jnp.int32))
    attended = outputs.reshape(row_count, seq_len, q_width)
    norms = norms.reshape(row_count, block_count, heads_q, query_block)
    log_norm = jnp.transpose(norms, (2, 0, 1, 3)).reshape(heads_q, row_count, seq_len)
    return attended, log_norm
```

```python
import functools
import math

import jax
import jax.numpy as jnp
from jax import lax
from jax.experimental import pallas as pl
from jax.experimental.pallas import tpu as pltpu
from jax.sharding import PartitionSpec as P

HEAD_SIZE = 128


def from_behind(value, axis, steps):
    count = lax.axis_size(axis)
    leading, last = (max(0, -steps), min(count, count - steps))
    return lax.ppermute(value, axis, [(source, source + steps) for source in range(leading, last)])


def doc_numbers(doc_ends, positions):
    return jnp.sum((doc_ends[:, None, :] <= positions[None, :, None]).astype(jnp.int32), axis=-1)


def per_device(queries, keys, values, lengths):
    local_q, local_k, local_v = (
        lax.all_to_all(queries, "heads", split_axis=2, concat_axis=1, tiled=True),
        lax.all_to_all(keys, "heads", split_axis=2, concat_axis=1, tiled=True),
        lax.all_to_all(values, "heads", split_axis=2, concat_axis=1, tiled=True),
    )
    row_count, tok_row, q_width = local_q.shape
    kv_heads = local_k.shape[2] // HEAD_SIZE
    per_group = q_width // (kv_heads * HEAD_SIZE)
    shards = lax.axis_size("dp")
    reach_blocks = shards // 8
    dp_index = lax.axis_index("dp")
    doc_ends = jnp.cumsum(lengths, axis=1)
    query_pos = dp_index * tok_row + jnp.arange(tok_row, dtype=jnp.int32)
    query_doc = doc_numbers(doc_ends, query_pos)
    doc_starts = jnp.max(
        jnp.where(doc_ends[:, None, :] <= query_pos[None, :, None], doc_ends[:, None, :], 0),
        axis=-1,
    )
    lowest = jnp.min(doc_starts)
    query_last = dp_index * tok_row + tok_row - 1
    query_heads = local_q.reshape(row_count, tok_row, kv_heads, per_group, HEAD_SIZE)
    score_scale = HEAD_SIZE ** (-0.5)

    def attend(state_now, key_block, value_block, anchor):
        run_max, run_sum, run_acc = state_now
        span_keys = key_block.shape[1]
        key_pos = anchor + jnp.arange(span_keys, dtype=jnp.int32)
        key_doc = doc_numbers(doc_ends, key_pos)
        visible = (
            (key_doc[:, None, :] == query_doc[:, :, None])
            & (key_pos[None, None, :] <= query_pos[None, :, None])
            & (key_pos[None, None, :] >= 0)
        )
        key_heads = key_block.reshape(row_count, span_keys, kv_heads, HEAD_SIZE)
        value_heads = value_block.reshape(row_count, span_keys, kv_heads, HEAD_SIZE)
        scores = (
            jnp.einsum(
                "rtkgd,rskd->kgrts", query_heads, key_heads, preferred_element_type=jnp.float32
            )
            * score_scale
        )
        masked = jnp.where(visible[None, None], scores, -1e30)
        new_max = jnp.maximum(run_max, jnp.max(masked, axis=-1))
        weights = jnp.where(visible[None, None], jnp.exp(masked - new_max[..., None]), 0.0)
        shrink = jnp.exp(run_max - new_max)
        run_sum = run_sum * shrink + jnp.sum(weights, axis=-1)
        partial_value = jnp.einsum(
            "kgrts,rskd->rtkgd",
            weights.astype(jnp.bfloat16),
            value_heads,
            preferred_element_type=jnp.float32,
        )
        run_acc = run_acc * jnp.transpose(shrink, (2, 3, 0, 1))[..., None] + partial_value
        return (new_max, run_sum, run_acc)

    def visit(state_now, key_block, value_block, anchor):
        key_end = anchor + key_block.shape[1] - 1
        needed = (anchor <= query_last) & (key_end >= lowest) & (key_end >= 0)
        result = lax.cond(
            needed,
            lambda carried: attend(carried, key_block, value_block, anchor),
            lambda carried: carried,
            state_now,
        )
        return result

    own_block = jnp.stack((local_k, local_v))
    shift_plan = []
    held_blocks = 1
    while 2 * held_blocks <= reach_blocks + 1:
        shift_plan.append((held_blocks, held_blocks))
        held_blocks = 2 * held_blocks
    if held_blocks < reach_blocks + 1:
        shift_plan.append((held_blocks, reach_blocks + 1 - held_blocks))
    window = own_block
    for distance, block_total in shift_plan:
        newest = window[:, :, window.shape[2] - block_total * tok_row :]
        earlier = from_behind(newest, "dp", distance)
        window = jnp.concatenate((earlier, window), axis=2)
    anchor_first = (dp_index - reach_blocks) * tok_row
    key_window = window[0]
    value_window = window[1]

    def advance(block_index, carried):
        key_block = lax.dynamic_slice_in_dim(key_window, block_index * tok_row, tok_row, 1)
        value_block = lax.dynamic_slice_in_dim(value_window, block_index * tok_row, tok_row, 1)
        return visit(carried, key_block, value_block, anchor_first + block_index * tok_row)

    initial = (
        jnp.full((kv_heads, per_group, row_count, tok_row), -1e30, jnp.float32),
        jnp.zeros((kv_heads, per_group, row_count, tok_row), jnp.float32),
        jnp.zeros((row_count, tok_row, kv_heads, per_group, HEAD_SIZE), jnp.float32),
    )
    folded = lax.fori_loop(0, reach_blocks + 1, advance, initial)
    run_max, run_sum, run_acc = folded
    scaled = run_acc / jnp.transpose(run_sum, (2, 3, 0, 1))[..., None]
    attended = scaled.astype(jnp.bfloat16).reshape(row_count, tok_row, q_width)
    spread = lax.all_to_all(attended, "heads", split_axis=1, concat_axis=2, tiled=True)
    log_norm = (run_max + jnp.log(run_sum)).reshape(kv_heads * per_group, row_count, tok_row)
    return (spread, log_norm)

MESH = pl.DeviceIdType.MESH


def fused_kernel(
    shards, q_ref, k_ref, v_ref, len_ref, out_ref, norm_ref,
    kv, qs, outs, lens, starts, columns, norms, held, inverse, stage, stage_half, k_all, v_all,
    sem_len, sem_own, recv_own, recv_x, recv_y, sends, recv_out, recv_norm, recv_stage, sem_load,
):
    rows, tok, q_width = q_ref.shape
    kv_half = k_ref.shape[2] // 2
    q_half = q_width // 2
    kv_heads = kv_half // HEAD_SIZE
    per_group = q_half // kv_half
    docs = len_ref.shape[1]
    span = 6 * tok
    dp = lax.axis_index("dp")
    index = lax.axis_index("heads")
    y = index // 2
    core = index % 2
    has_prev = dp > 0
    has_next = dp < shards - 1

    def at(d, chip, c):
        return {"dp": d, "heads": 2 * chip + c}

    def remote(src, dst, send, recv, device):
        return pltpu.make_async_remote_copy(
            src_ref=src, dst_ref=dst, send_sem=send, recv_sem=recv,
            device_id=device, device_id_type=MESH,
        )

    def drain(ref, sem):
        pltpu.make_async_copy(ref, ref, sem).wait()

    barrier = pltpu.get_barrier_semaphore()

    def greet(device):
        pl.semaphore_signal(barrier, inc=1, device_id=device, device_id_type=MESH)

    @pl.when(has_prev)
    def _():
        greet(at(dp - 1, y, 0))
        greet(at(dp - 1, y, 1))

    greet(at(dp, 1 - y, 0))
    greet(at(dp, 1 - y, 1))
    greet(at(dp, y, 1 - core))

    def part(ref, c):
        width = ref.shape[2] // 2
        return (slice(None), pl.ds(pl.multiple_of(c * width, width), width))

    load_k = pltpu.make_async_copy(k_ref, k_all, sem_load.at[0])
    load_v = pltpu.make_async_copy(v_ref, v_all, sem_load.at[1])
    load_k.start()
    load_v.start()

    len_copy = pltpu.make_async_copy(len_ref, lens, sem_len)
    len_copy.start()
    mine = (
        pltpu.make_async_copy(q_ref.at[(slice(None),) + part(q_ref, core)], qs.at[:, core], sem_own),
        pltpu.make_async_copy(k_ref.at[(slice(None),) + part(k_ref, core)], kv.at[:, 0, 4 + core], sem_own),
        pltpu.make_async_copy(v_ref.at[(slice(None),) + part(v_ref, core)], kv.at[:, 1, 4 + core], sem_own),
    )
    for copy in mine:
        copy.start()

    pl.semaphore_wait(
        barrier, 3 + 2 * has_next.astype(jnp.int32)
    )

    def group(r, which):
        if which == 0:
            return 2 * r // rows
        return 2 + (2 * r // rows) + jnp.maximum(r - (rows - 3), 0)

    def send_rows(which, ref):
        def send_row(r, carry):
            @pl.when(has_next)
            def _():
                for c in (0, 1):
                    remote(
                        ref.at[(r,) + part(ref, c)], kv.at[r, which, core],
                        sends, recv_x.at[r, which], at(dp + 1, y, c),
                    ).start()

            @pl.when(y == 0)
            def _():
                for c in (0, 1):
                    remote(
                        ref.at[(r,) + part(ref, c)], kv.at[r, which, 2 + core],
                        sends, recv_y.at[group(r, which)], at(dp, 1, c),
                    ).start()

            return carry

        lax.fori_loop(0, rows, send_row, 0)

    load_k.wait()
    send_rows(0, k_all)
    load_v.wait()

    across = jnp.logical_and(has_next, y == 1)
    onward = jnp.logical_and(has_next, y == 0)

    @pl.when(across)
    def _():
        for c in (0, 1):
            remote(
                v_all.at[(rows - 1,) + part(v_ref, c)], stage.at[core],
                sends, recv_stage.at[0], at(dp, 0, c),
            ).start()
            remote(
                v_all.at[rows - 2, :, pl.ds(c * kv_half, kv_half // 2)], stage_half.at[core],
                sends, recv_stage.at[1], at(dp, 0, c),
            ).start()

    send_rows(1, v_all)

    partner = at(dp, y, 1 - core)
    theirs = (
        remote(q_ref.at[(slice(None),) + part(q_ref, 1 - core)], qs.at[:, core], sends, recv_own, partner),
        remote(k_ref.at[(slice(None),) + part(k_ref, 1 - core)], kv.at[:, 0, 4 + core], sends, recv_own, partner),
        remote(v_ref.at[(slice(None),) + part(v_ref, 1 - core)], kv.at[:, 1, 4 + core], sends, recv_own, partner),
    )
    for copy in theirs:
        copy.start()

    @pl.when(jnp.logical_not(has_prev))
    def _():
        kv[:, :, 0:2] = jnp.zeros((rows, 2, 2, tok, kv_half), kv.dtype)

        @pl.when(y == 0)
        def _():
            kv[:, :, 2:4] = jnp.zeros((rows, 2, 2, tok, kv_half), kv.dtype)

    len_copy.wait()
    base = (4 * dp + 2 * y) * tok
    upto = lax.broadcasted_iota(jnp.int32, (docs, docs), 0) <= lax.broadcasted_iota(jnp.int32, (docs, docs), 1)
    ends = jnp.dot(
        lens[...].astype(jnp.float32), upto.astype(jnp.float32),
        precision=lax.Precision.HIGHEST, preferred_element_type=jnp.float32,
    )
    query = (lax.broadcasted_iota(jnp.int32, (2 * tok, docs), 0) + base).astype(jnp.float32)
    for r in range(rows):
        row_ends = ends[r : r + 1, :]
        first = jnp.max(jnp.where(row_ends <= query, row_ends, 0.0), axis=1, keepdims=True)
        starts[r] = jnp.broadcast_to(first.astype(jnp.int32) - (base - 4 * tok), (2 * tok, HEAD_SIZE))


    @pl.when(onward)
    def _():
        drain(stage_half, recv_stage.at[1])
        remote(
            stage_half, kv.at[rows - 2, 1, 2:4, :, 0 : kv_half // 2], sends,
            recv_y.at[group(rows - 2, 1)], at(dp + 1, 0, core),
        ).start()
        drain(stage, recv_stage.at[0])
        remote(
            stage, kv.at[rows - 1, 1, 2:4], sends, recv_y.at[group(rows - 1, 1)],
            at(dp + 1, 0, core),
        ).start()

    factor = HEAD_SIZE ** (-0.5)
    power = factor / math.log(2.0)
    lane = lax.broadcasted_iota(jnp.int32, (2 * tok, HEAD_SIZE), 1)

    q_heads = kv_heads * per_group
    half = q_heads // 2
    spot = pl.ds(pl.multiple_of(y * 2 * tok, 2 * tok), 2 * tok)

    def take(r, which):
        @pl.when(has_prev)
        def _():
            drain(kv.at[r, which, 0:2], recv_x.at[r, which])
            relayed = y == 1
            if which == 1:
                relayed = jnp.logical_and(relayed, r < rows - 2)

                @pl.when(jnp.logical_and(y == 1, r == rows - 2))
                def _():
                    rest = slice(kv_half // 2, kv_half)
                    remote(
                        kv.at[r, which, 0:2, :, rest], kv.at[r, which, 2:4, :, rest],
                        sends, recv_y.at[group(r, which)], at(dp, 0, core),
                    ).start()

            @pl.when(relayed)
            def _():
                remote(
                    kv.at[r, which, 0:2], kv.at[r, which, 2:4],
                    sends, recv_y.at[group(r, which)], at(dp, 0, core),
                ).start()

    def gathered(first, count, which):
        @pl.when(jnp.logical_or(has_prev, y == 1))
        def _():
            drain(kv.at[first : first + count, which, 2:4], recv_y.at[group(first, which)])

    def send_norms():
        turned = columns[...].T
        norms[...] = turned[0 : q_heads * rows].reshape(q_heads, rows, 2 * tok)
        for t in (0, 1):
            own = jnp.logical_and(y == core, core == t)
            source = norms.at[t * half : (t + 1) * half]

            @pl.when(own)
            def _():
                pltpu.make_async_copy(source, norm_ref.at[:, :, spot], recv_norm).start()

            @pl.when(jnp.logical_not(own))
            def _():
                remote(source, norm_ref.at[:, :, spot], sends, recv_norm, at(dp, core, t)).start()

    def score_row(r):
        key_at = lax.broadcasted_iota(jnp.int32, (2 * tok, span), 1)
        last = lax.broadcasted_iota(jnp.int32, (2 * tok, span), 0) + 4 * tok
        first = starts[r][:, 0:1]
        visible = (key_at >= first) & (key_at <= last)
        found = columns[...]
        for j in range(q_heads):
            head = j // per_group
            at_kv = slice(head * HEAD_SIZE, (head + 1) * HEAD_SIZE)
            at_q = slice(j * HEAD_SIZE, (j + 1) * HEAD_SIZE)
            keys = kv[r, 0, :, :, at_kv].reshape(span, HEAD_SIZE)
            query_rows = qs[r, :, :, at_q].reshape(2 * tok, HEAD_SIZE)
            products = lax.dot_general(
                query_rows, keys, (((1,), (1,)), ((), ())),
                preferred_element_type=jnp.float32,
            )
            masked = jnp.where(visible, products, -1e30)
            top = jnp.max(masked, axis=1, keepdims=True)
            weights = jnp.exp2((masked - top) * power)
            total = jnp.sum(weights, axis=1, keepdims=True)
            held[r, j] = weights.astype(jnp.bfloat16)
            inverse[r, j] = jnp.broadcast_to(1.0 / total, (2 * tok, HEAD_SIZE))
            found = jnp.where(lane == j * rows + r, top * factor + jnp.log(total), found)
        columns[...] = found

    def mix_row(r):
        for j in range(q_heads):
            head = j // per_group
            at_kv = slice(head * HEAD_SIZE, (head + 1) * HEAD_SIZE)
            at_q = slice(j * HEAD_SIZE, (j + 1) * HEAD_SIZE)
            vals = kv[r, 1, :, :, at_kv].reshape(span, HEAD_SIZE)
            mixed = jnp.dot(held[r, j], vals, preferred_element_type=jnp.float32)
            outs[r, :, :, at_q] = (
                (mixed * inverse[r, j]).astype(jnp.bfloat16).reshape(2, tok, HEAD_SIZE)
            )
        place = (r, slice(None), pl.ds(pl.multiple_of(core * q_half, q_half), q_half))
        remote(
            outs.at[r, 1 - core], out_ref.at[place], sends, recv_out, partner
        ).start()
        pltpu.make_async_copy(outs.at[r, core], out_ref.at[place], recv_out).start()

    part_rows = rows // 2

    def each(body):
        def step(i, carry):
            body(i)
            return carry

        lax.fori_loop(0, part_rows, step, 0)

    def first_scores(i):
        take(part_rows + i, 0)
        score_row(i)

    def later_scores(i):
        take(i, 1)
        score_row(part_rows + i)

    def first_mixes(i):
        take(part_rows + i, 1)
        mix_row(i)

    columns[...] = jnp.zeros(columns.shape, jnp.float32)
    each(lambda i: take(i, 0))
    drain(qs, sem_own)
    drain(qs, recv_own)
    gathered(0, part_rows, 0)
    each(first_scores)
    gathered(part_rows, part_rows, 0)
    each(later_scores)
    send_norms()
    gathered(0, part_rows, 1)
    each(first_mixes)
    gathered(part_rows, part_rows - 2, 1)
    for r in range(part_rows, rows - 2):
        mix_row(r)
    for r in (rows - 2, rows - 1):
        gathered(r, 1, 1)
        mix_row(r)

    drain(qs, sends)

    @pl.when(has_next)
    def _():
        drain(kv.at[:, :, 0:2], sends)
        drain(stage, sends)
        drain(stage_half, sends)

    @pl.when(y == 0)
    def _():
        drain(kv.at[:, :, 2:4], sends)

    @pl.when(jnp.logical_and(has_prev, y == 1))
    def _():
        drain(kv.at[:, 0, 2:4], sends)
        drain(kv.at[0 : rows - 2, 1, 2:4], sends)
        drain(kv.at[0, 1, 2:4, :, 0 : kv_half // 2], sends)

    drain(outs.at[:, 0], sends)
    drain(norms.at[0:half], sends)

    @pl.when(y != core)
    def _():
        drain(norms.at[0:half], sends)

    drain(outs, recv_out)
    drain(norms, recv_norm)


def store_kernel(out_ref, norm_ref, out_to, norm_to, sems):
    copies = [
        pltpu.make_async_copy(norm_ref, norm_to, sems.at[1]),
        pltpu.make_async_copy(out_ref, out_to, sems.at[0]),
    ]
    for copy in copies:
        copy.start()
    for copy in copies:
        copy.wait()


def store(attended, log_norm):
    return pl.pallas_call(
        store_kernel,
        out_shape=(
            pltpu.HBM(attended.shape, attended.dtype),
            pltpu.HBM(log_norm.shape, log_norm.dtype),
        ),
        in_specs=[pl.BlockSpec(memory_space=pl.ANY)] * 2,
        out_specs=(pl.BlockSpec(memory_space=pl.ANY),) * 2,
        scratch_shapes=[pltpu.SemaphoreType.DMA((2,))],
    )(*(pltpu.with_memory_space_constraint(a, pltpu.VMEM) for a in (attended, log_norm)))


def fused(queries, keys, values, lengths):
    rows, tok, q_width = queries.shape
    kv_width = keys.shape[2]
    heads = lax.axis_size("heads")
    q_heads = q_width // HEAD_SIZE
    dma = pltpu.SemaphoreType.DMA
    results = pl.pallas_call(
        functools.partial(fused_kernel, lax.axis_size("dp")),
        out_shape=(
            pltpu.VMEM((rows, tok, q_width), jnp.bfloat16),
            pltpu.VMEM((q_heads // heads, rows, heads * tok), jnp.float32),
        ),
        in_specs=[pl.BlockSpec(memory_space=pltpu.HBM)] * 4,
        out_specs=(pl.BlockSpec(memory_space=pl.ANY),) * 2,
        scratch_shapes=[
            pltpu.VMEM((rows, 2, 6, tok, kv_width // 2), jnp.bfloat16),
            pltpu.VMEM((rows, 2, tok, q_width // 2), jnp.bfloat16),
            pltpu.VMEM((rows, 2, tok, q_width // 2), jnp.bfloat16),
            pltpu.VMEM(lengths.shape, jnp.int32),
            pltpu.VMEM((rows, 2 * tok, HEAD_SIZE), jnp.int32),
            pltpu.VMEM((2 * tok, HEAD_SIZE), jnp.float32),
            pltpu.VMEM((q_heads // 2, rows, 2 * tok), jnp.float32),
            pltpu.VMEM((rows, q_heads // 2, 2 * tok, 6 * tok), jnp.bfloat16),
            pltpu.VMEM((rows, q_heads // 2, 2 * tok, HEAD_SIZE), jnp.float32),
            pltpu.VMEM((2, tok, kv_width // 2), jnp.bfloat16),
            pltpu.VMEM((2, tok, kv_width // 4), jnp.bfloat16),
            pltpu.VMEM(keys.shape, jnp.bfloat16),
            pltpu.VMEM(values.shape, jnp.bfloat16),
            dma, dma, dma, dma((rows, 2)), dma((6,)), dma, dma, dma, dma((2,)), dma((2,)),
        ],
        compiler_params=pltpu.CompilerParams(
            collective_id=0, has_side_effects=True, vmem_limit_bytes=48 * 1024 * 1024
        ),
    )(*(pltpu.with_memory_space_constraint(a, pltpu.HBM) for a in (queries, keys, values, lengths)))
    return store(*results)


def dispatch(queries, keys, values, lengths):
    heads, shards = lax.axis_size("heads"), lax.axis_size("dp")
    tok = queries.shape[1]
    suited = (
        heads == 4
        and shards // 8 == 1
        and shards > 2
        and 2 * tok == HEAD_SIZE
        and keys.shape[2] == heads * HEAD_SIZE
        and queries.shape[0] % 2 == 0
        and queries.shape[0] >= 8
        and queries.shape[2] * queries.shape[0] <= 2 * HEAD_SIZE * HEAD_SIZE
    )
    return (fused if suited else per_device)(queries, keys, values, lengths)


def solution(mesh):
    in_specs = (
        P(None, ("dp", "heads"), None),
        P(None, ("dp", "heads"), None),
        P(None, ("dp", "heads"), None),
        P(),
    )
    out_specs = (P(None, ("dp", "heads"), None), P("heads", None, "dp"))
    return jax.shard_map(
        dispatch, mesh=mesh, in_specs=in_specs, out_specs=out_specs, check_vma=False
    )
```

```python
import functools
import math

import jax
import jax.numpy as jnp
from jax import lax
from jax.experimental import pallas as pl
from jax.experimental.pallas import tpu as pltpu
from jax.sharding import PartitionSpec as P

HEAD_SIZE = 128


def from_behind(value, axis, steps):
    count = lax.axis_size(axis)
    leading, last = (max(0, -steps), min(count, count - steps))
    return lax.ppermute(value, axis, [(source, source + steps) for source in range(leading, last)])


def doc_numbers(doc_ends, positions):
    return jnp.sum((doc_ends[:, None, :] <= positions[None, :, None]).astype(jnp.int32), axis=-1)


def per_device(queries, keys, values, lengths):
    local_q, local_k, local_v = (
        lax.all_to_all(queries, "heads", split_axis=2, concat_axis=1, tiled=True),
        lax.all_to_all(keys, "heads", split_axis=2, concat_axis=1, tiled=True),
        lax.all_to_all(values, "heads", split_axis=2, concat_axis=1, tiled=True),
    )
    row_count, tok_row, q_width = local_q.shape
    kv_heads = local_k.shape[2] // HEAD_SIZE
    per_group = q_width // (kv_heads * HEAD_SIZE)
    shards = lax.axis_size("dp")
    reach_blocks = shards // 8
    dp_index = lax.axis_index("dp")
    doc_ends = jnp.cumsum(lengths, axis=1)
    query_pos = dp_index * tok_row + jnp.arange(tok_row, dtype=jnp.int32)
    query_doc = doc_numbers(doc_ends, query_pos)
    doc_starts = jnp.max(
        jnp.where(doc_ends[:, None, :] <= query_pos[None, :, None], doc_ends[:, None, :], 0),
        axis=-1,
    )
    lowest = jnp.min(doc_starts)
    query_last = dp_index * tok_row + tok_row - 1
    query_heads = local_q.reshape(row_count, tok_row, kv_heads, per_group, HEAD_SIZE)
    score_scale = HEAD_SIZE ** (-0.5)

    def attend(state_now, key_block, value_block, anchor):
        run_max, run_sum, run_acc = state_now
        span_keys = key_block.shape[1]
        key_pos = anchor + jnp.arange(span_keys, dtype=jnp.int32)
        key_doc = doc_numbers(doc_ends, key_pos)
        visible = (
            (key_doc[:, None, :] == query_doc[:, :, None])
            & (key_pos[None, None, :] <= query_pos[None, :, None])
            & (key_pos[None, None, :] >= 0)
        )
        key_heads = key_block.reshape(row_count, span_keys, kv_heads, HEAD_SIZE)
        value_heads = value_block.reshape(row_count, span_keys, kv_heads, HEAD_SIZE)
        scores = (
            jnp.einsum(
                "rtkgd,rskd->kgrts", query_heads, key_heads, preferred_element_type=jnp.float32
            )
            * score_scale
        )
        masked = jnp.where(visible[None, None], scores, -1e30)
        new_max = jnp.maximum(run_max, jnp.max(masked, axis=-1))
        weights = jnp.where(visible[None, None], jnp.exp(masked - new_max[..., None]), 0.0)
        shrink = jnp.exp(run_max - new_max)
        run_sum = run_sum * shrink + jnp.sum(weights, axis=-1)
        partial_value = jnp.einsum(
            "kgrts,rskd->rtkgd",
            weights.astype(jnp.bfloat16),
            value_heads,
            preferred_element_type=jnp.float32,
        )
        run_acc = run_acc * jnp.transpose(shrink, (2, 3, 0, 1))[..., None] + partial_value
        return (new_max, run_sum, run_acc)

    def visit(state_now, key_block, value_block, anchor):
        key_end = anchor + key_block.shape[1] - 1
        needed = (anchor <= query_last) & (key_end >= lowest) & (key_end >= 0)
        result = lax.cond(
            needed,
            lambda carried: attend(carried, key_block, value_block, anchor),
            lambda carried: carried,
            state_now,
        )
        return result

    own_block = jnp.stack((local_k, local_v))
    shift_plan = []
    held_blocks = 1
    while 2 * held_blocks <= reach_blocks + 1:
        shift_plan.append((held_blocks, held_blocks))
        held_blocks = 2 * held_blocks
    if held_blocks < reach_blocks + 1:
        shift_plan.append((held_blocks, reach_blocks + 1 - held_blocks))
    window = own_block
    for distance, block_total in shift_plan:
        newest = window[:, :, window.shape[2] - block_total * tok_row :]
        earlier = from_behind(newest, "dp", distance)
        window = jnp.concatenate((earlier, window), axis=2)
    anchor_first = (dp_index - reach_blocks) * tok_row
    key_window = window[0]
    value_window = window[1]

    def advance(block_index, carried):
        key_block = lax.dynamic_slice_in_dim(key_window, block_index * tok_row, tok_row, 1)
        value_block = lax.dynamic_slice_in_dim(value_window, block_index * tok_row, tok_row, 1)
        return visit(carried, key_block, value_block, anchor_first + block_index * tok_row)

    initial = (
        jnp.full((kv_heads, per_group, row_count, tok_row), -1e30, jnp.float32),
        jnp.zeros((kv_heads, per_group, row_count, tok_row), jnp.float32),
        jnp.zeros((row_count, tok_row, kv_heads, per_group, HEAD_SIZE), jnp.float32),
    )
    folded = lax.fori_loop(0, reach_blocks + 1, advance, initial)
    run_max, run_sum, run_acc = folded
    scaled = run_acc / jnp.transpose(run_sum, (2, 3, 0, 1))[..., None]
    attended = scaled.astype(jnp.bfloat16).reshape(row_count, tok_row, q_width)
    spread = lax.all_to_all(attended, "heads", split_axis=1, concat_axis=2, tiled=True)
    log_norm = (run_max + jnp.log(run_sum)).reshape(kv_heads * per_group, row_count, tok_row)
    return (spread, log_norm)

MESH = pl.DeviceIdType.MESH


def fused_kernel(
    shards, q_ref, k_ref, v_ref, len_ref, out_ref, norm_ref,
    kv, qs, outs, lens, starts, columns, norms, held, inverse, stage, stage_late, detour, k_all, v_all,
    sem_len, sem_own, recv_own, recv_x, recv_y, sends, recv_out, recv_norm, recv_stage, recv_detour, sem_load, landed,
):
    rows, tok, q_width = q_ref.shape
    kv_half = k_ref.shape[2] // 2
    q_half = q_width // 2
    kv_heads = kv_half // HEAD_SIZE
    per_group = q_half // kv_half
    docs = len_ref.shape[1]
    span = 6 * tok
    dp = lax.axis_index("dp")
    index = lax.axis_index("heads")
    y = index // 2
    core = index % 2
    has_prev = dp > 0
    has_next = dp < shards - 1
    odd = dp % 2 == 1
    even = dp % 2 == 0
    around = rows // 4
    lands = jnp.logical_and(y == 0, jnp.logical_and(even, has_prev))
    detours = jnp.logical_and(y == 0, jnp.logical_and(odd, has_next))
    passes = jnp.logical_and(y == 0, dp == 0)
    sent_round = jnp.where(detours, around, 0)
    landings = range(2, shards, 2)
    half_head = kv_half // 2

    def at(d, chip, c):
        return {"dp": d, "heads": 2 * chip + c}

    def remote(src, dst, send, recv, device):
        return pltpu.make_async_remote_copy(
            src_ref=src, dst_ref=dst, send_sem=send, recv_sem=recv,
            device_id=device, device_id_type=MESH,
        )

    def drain(ref, sem):
        pltpu.make_async_copy(ref, ref, sem).wait()

    barrier = pltpu.get_barrier_semaphore()

    def greet(device):
        pl.semaphore_signal(barrier, inc=1, device_id=device, device_id_type=MESH)

    @pl.when(has_prev)
    def _():
        greet(at(dp - 1, y, 0))
        greet(at(dp - 1, y, 1))

    greet(at(dp, 1 - y, 0))
    greet(at(dp, 1 - y, 1))
    greet(at(dp, y, 1 - core))

    @pl.when(passes)
    def _():
        for d in landings:
            greet(at(d - 1, 0, core))
            greet(at(d, 0, 0))
            greet(at(d, 0, 1))

    def part(ref, c):
        width = ref.shape[2] // 2
        return (slice(None), pl.ds(pl.multiple_of(c * width, width), width))

    load_k = pltpu.make_async_copy(k_ref, k_all, sem_load.at[0])
    load_v = pltpu.make_async_copy(v_ref, v_all, sem_load.at[1])
    load_k.start()
    load_v.start()

    len_copy = pltpu.make_async_copy(len_ref, lens, sem_len)
    len_copy.start()
    mine = (
        pltpu.make_async_copy(q_ref.at[(slice(None),) + part(q_ref, core)], qs.at[:, core], sem_own),
        pltpu.make_async_copy(k_ref.at[(slice(None),) + part(k_ref, core)], kv.at[:, 0, 4 + core], sem_own),
        pltpu.make_async_copy(v_ref.at[(slice(None),) + part(v_ref, core)], kv.at[:, 1, 4 + core], sem_own),
    )
    for copy in mine:
        copy.start()

    pl.semaphore_wait(
        barrier,
        3 + 2 * has_next.astype(jnp.int32) + detours.astype(jnp.int32) + 2 * lands.astype(jnp.int32),
    )

    @pl.when(lands)
    def _():
        for c in (0, 1):
            pl.semaphore_signal(landed, inc=1, device_id=at(0, 0, c), device_id_type=MESH)

    def group(r, which):
        if which == 0:
            return 2 * r // rows
        return 2 + jnp.maximum(r - rows // 2 + 1, 0)

    def send_rows(which, ref):
        def send_row(r, carry):
            straight = has_next
            if which == 1:
                straight = jnp.logical_and(has_next, r < rows - sent_round)

            @pl.when(straight)
            def _():
                for c in (0, 1):
                    remote(
                        ref.at[(r,) + part(ref, c)], kv.at[r, which, core],
                        sends, recv_x.at[r, which], at(dp + 1, y, c),
                    ).start()

            @pl.when(y == 0)
            def _():
                for c in (0, 1):
                    remote(
                        ref.at[(r,) + part(ref, c)], kv.at[r, which, 2 + core],
                        sends, recv_y.at[group(r, which)], at(dp, 1, c),
                    ).start()

            return carry

        lax.fori_loop(0, rows, send_row, 0)

    load_k.wait()
    send_rows(0, k_all)
    load_v.wait()

    across = jnp.logical_and(has_next, y == 1)
    onward = jnp.logical_and(has_next, y == 0)

    @pl.when(across)
    def _():
        for c in (0, 1):
            remote(
                v_all.at[(rows - 1,) + part(v_ref, c)], stage.at[core],
                sends, recv_stage.at[0], at(dp, 0, c),
            ).start()

            def late(skip):
                width = slice(skip * half_head, (skip + 1) * half_head)
                remote(
                    v_all.at[rows - 2, :, pl.ds(c * kv_half + skip * half_head, half_head)],
                    stage_late.at[core, :, width], sends, recv_stage.at[1], at(dp, 0, c),
                ).start()

            late(0)

            @pl.when(odd)
            def _():
                late(1)

    send_rows(1, v_all)

    @pl.when(detours)
    def _():
        slot = (dp - 1) // 2
        remote(
            v_all.at[rows - around : rows], detour.at[slot], sends, recv_detour.at[slot], at(0, 0, core)
        ).start()

    partner = at(dp, y, 1 - core)
    theirs = (
        remote(q_ref.at[(slice(None),) + part(q_ref, 1 - core)], qs.at[:, core], sends, recv_own, partner),
        remote(k_ref.at[(slice(None),) + part(k_ref, 1 - core)], kv.at[:, 0, 4 + core], sends, recv_own, partner),
        remote(v_ref.at[(slice(None),) + part(v_ref, 1 - core)], kv.at[:, 1, 4 + core], sends, recv_own, partner),
    )
    for copy in theirs:
        copy.start()

    @pl.when(jnp.logical_not(has_prev))
    def _():
        kv[:, :, 0:2] = jnp.zeros((rows, 2, 2, tok, kv_half), kv.dtype)

        @pl.when(y == 0)
        def _():
            kv[:, :, 2:4] = jnp.zeros((rows, 2, 2, tok, kv_half), kv.dtype)

    len_copy.wait()
    base = (4 * dp + 2 * y) * tok
    upto = lax.broadcasted_iota(jnp.int32, (docs, docs), 0) <= lax.broadcasted_iota(jnp.int32, (docs, docs), 1)
    ends = jnp.dot(
        lens[...].astype(jnp.float32), upto.astype(jnp.float32),
        precision=lax.Precision.HIGHEST, preferred_element_type=jnp.float32,
    )
    query = (lax.broadcasted_iota(jnp.int32, (2 * tok, docs), 0) + base).astype(jnp.float32)
    for r in range(rows):
        row_ends = ends[r : r + 1, :]
        first = jnp.max(jnp.where(row_ends <= query, row_ends, 0.0), axis=1, keepdims=True)
        starts[r] = jnp.broadcast_to(first.astype(jnp.int32) - (base - 4 * tok), (2 * tok, HEAD_SIZE))


    @pl.when(onward)
    def _():
        @pl.when(odd)
        def _():
            drain(stage_late, recv_stage.at[1])
            remote(
                stage_late, kv.at[rows - 2, 1, 2:4], sends, recv_y.at[group(rows - 2, 1)],
                at(dp + 1, 0, core),
            ).start()

        @pl.when(even)
        def _():
            drain(stage_late.at[:, :, 0:half_head], recv_stage.at[1])
            remote(
                stage_late.at[:, :, 0:half_head], kv.at[rows - 2, 1, 2:4, :, 0:half_head], sends,
                recv_y.at[group(rows - 2, 1)], at(dp + 1, 0, core),
            ).start()

        drain(stage, recv_stage.at[0])
        remote(
            stage, kv.at[rows - 1, 1, 2:4], sends, recv_y.at[group(rows - 1, 1)],
            at(dp + 1, 0, core),
        ).start()

    def pass_on():
        pl.semaphore_wait(landed, 2 * len(landings))
        for slot, d in enumerate(landings):
            drain(detour.at[slot], recv_detour.at[slot])
            for i in range(around):
                for c in (0, 1):
                    remote(
                        detour.at[slot, i, :, c * kv_half : (c + 1) * kv_half],
                        kv.at[rows - around + i, 1, core], sends,
                        recv_x.at[rows - around + i, 1], at(d, 0, c),
                    ).start()

    factor = HEAD_SIZE ** (-0.5)
    power = factor / math.log(2.0)
    lane = lax.broadcasted_iota(jnp.int32, (2 * tok, HEAD_SIZE), 1)

    q_heads = kv_heads * per_group
    half = q_heads // 2
    spot = pl.ds(pl.multiple_of(y * 2 * tok, 2 * tok), 2 * tok)

    def take(r, which):
        @pl.when(has_prev)
        def _():
            drain(kv.at[r, which, 0:2], recv_x.at[r, which])
            relayed = y == 1
            if which == 1:
                relayed = jnp.logical_and(relayed, r < rows - 2)

                @pl.when(jnp.logical_and(jnp.logical_and(y == 1, odd), r == rows - 2))
                def _():
                    rest = slice(half_head, kv_half)
                    remote(
                        kv.at[r, which, 0:2, :, rest], kv.at[r, which, 2:4, :, rest],
                        sends, recv_y.at[group(r, which)], at(dp, 0, core),
                    ).start()

            @pl.when(relayed)
            def _():
                remote(
                    kv.at[r, which, 0:2], kv.at[r, which, 2:4],
                    sends, recv_y.at[group(r, which)], at(dp, 0, core),
                ).start()

    def gathered(first, count, which):
        @pl.when(jnp.logical_or(has_prev, y == 1))
        def _():
            drain(kv.at[pl.ds(first, count), which, 2:4], recv_y.at[group(first, which)])

    def send_norms():
        turned = columns[...].T
        norms[...] = turned[0 : q_heads * rows].reshape(q_heads, rows, 2 * tok)
        for t in (0, 1):
            own = jnp.logical_and(y == core, core == t)
            source = norms.at[t * half : (t + 1) * half]

            @pl.when(own)
            def _():
                pltpu.make_async_copy(source, norm_ref.at[:, :, spot], recv_norm).start()

            @pl.when(jnp.logical_not(own))
            def _():
                remote(source, norm_ref.at[:, :, spot], sends, recv_norm, at(dp, core, t)).start()

    def score_row(r):
        key_at = lax.broadcasted_iota(jnp.int32, (2 * tok, span), 1)
        last = lax.broadcasted_iota(jnp.int32, (2 * tok, span), 0) + 4 * tok
        first = starts[r][:, 0:1]
        visible = (key_at >= first) & (key_at <= last)
        found = columns[...]
        for j in range(q_heads):
            head = j // per_group
            at_kv = slice(head * HEAD_SIZE, (head + 1) * HEAD_SIZE)
            at_q = slice(j * HEAD_SIZE, (j + 1) * HEAD_SIZE)
            keys = kv[r, 0, :, :, at_kv].reshape(span, HEAD_SIZE)
            query_rows = qs[r, :, :, at_q].reshape(2 * tok, HEAD_SIZE)
            products = lax.dot_general(
                query_rows, keys, (((1,), (1,)), ((), ())),
                preferred_element_type=jnp.float32,
            )
            masked = jnp.where(visible, products, -1e30)
            top = jnp.max(masked, axis=1, keepdims=True)
            weights = jnp.exp2((masked - top) * power)
            total = jnp.sum(weights, axis=1, keepdims=True)
            held[r, j] = weights.astype(jnp.bfloat16)
            inverse[r, j] = jnp.broadcast_to(1.0 / total, (2 * tok, HEAD_SIZE))
            found = jnp.where(lane == j * rows + r, top * factor + jnp.log(total), found)
        columns[...] = found

    def mix(r, rows_of, place):
        for j in range(q_heads):
            head = j // per_group
            at_kv = slice(head * HEAD_SIZE, (head + 1) * HEAD_SIZE)
            at_q = slice(j * HEAD_SIZE, (j + 1) * HEAD_SIZE)
            vals = kv[r, 1, :, :, at_kv].reshape(span, HEAD_SIZE)
            mixed = jnp.dot(held[r, j, rows_of], vals, preferred_element_type=jnp.float32)
            result = (mixed * inverse[r, j, rows_of]).astype(jnp.bfloat16)
            outs[r, place, :, at_q] = result.reshape(-1, tok, HEAD_SIZE) if place == slice(None) else result

    columns_of = pl.ds(pl.multiple_of(core * q_half, q_half), q_half)

    def send_out(r):
        remote(
            outs.at[r, 1 - core], out_ref.at[r, :, columns_of], sends, recv_out, partner
        ).start()

    def keep_out(r):
        pltpu.make_async_copy(outs.at[r, core], out_ref.at[r, :, columns_of], recv_out).start()

    def mix_row(r):
        mix(r, slice(None), slice(None))
        send_out(r)
        keep_out(r)

    def mix_split(r):
        for c, finish in ((1 - core, send_out), (core, keep_out)):
            mix(r, pl.ds(pl.multiple_of(c * tok, tok), tok), c)
            finish(r)

    part_rows = rows // 2

    def each(body):
        def step(i, carry):
            body(i)
            return carry

        lax.fori_loop(0, part_rows, step, 0)

    def first_scores(i):
        take(part_rows + i, 0)
        score_row(i)

    def later_scores(i):
        take(i, 1)
        score_row(part_rows + i)

    def first_mixes(i):
        take(part_rows + i, 1)
        mix_row(i)

    columns[...] = jnp.zeros(columns.shape, jnp.float32)
    each(lambda i: take(i, 0))
    pl.when(passes)(pass_on)
    drain(qs, sem_own)
    drain(qs, recv_own)
    gathered(0, part_rows, 0)
    each(first_scores)
    gathered(part_rows, part_rows, 0)
    each(later_scores)
    send_norms()
    gathered(0, part_rows, 1)
    each(first_mixes)
    late = even.astype(jnp.int32)
    for r in [*range(part_rows, rows - 3), rows - 3 + late, rows - 1]:
        gathered(r, 1, 1)
        mix_row(r)
    gathered(rows - 2 - late, 1, 1)
    mix_split(rows - 2 - late)

    drain(qs, sends)

    @pl.when(has_next)
    def _():
        drain(kv.at[:, :, 0:2], sends)
        drain(stage, sends)
        drain(stage_late.at[:, :, 0:half_head], sends)

        @pl.when(odd)
        def _():
            drain(stage_late.at[:, :, 0:half_head], sends)

    @pl.when(y == 0)
    def _():
        drain(kv.at[:, :, 2:4], sends)

    @pl.when(jnp.logical_and(has_prev, y == 1))
    def _():
        drain(kv.at[:, 0, 2:4], sends)
        drain(kv.at[0 : rows - 2, 1, 2:4], sends)

        @pl.when(odd)
        def _():
            drain(kv.at[0, 1, 2:4, :, 0:half_head], sends)

    @pl.when(passes)
    def _():
        drain(detour, sends)

    drain(outs.at[:, 0], sends)
    drain(norms.at[0:half], sends)

    @pl.when(y != core)
    def _():
        drain(norms.at[0:half], sends)

    drain(outs, recv_out)
    drain(norms, recv_norm)


def store_kernel(out_ref, norm_ref, out_to, norm_to, sems):
    copies = [
        pltpu.make_async_copy(norm_ref, norm_to, sems.at[1]),
        pltpu.make_async_copy(out_ref, out_to, sems.at[0]),
    ]
    for copy in copies:
        copy.start()
    for copy in copies:
        copy.wait()


def store(attended, log_norm):
    return pl.pallas_call(
        store_kernel,
        out_shape=(
            pltpu.HBM(attended.shape, attended.dtype),
            pltpu.HBM(log_norm.shape, log_norm.dtype),
        ),
        in_specs=[pl.BlockSpec(memory_space=pl.ANY)] * 2,
        out_specs=(pl.BlockSpec(memory_space=pl.ANY),) * 2,
        scratch_shapes=[pltpu.SemaphoreType.DMA((2,))],
    )(*(pltpu.with_memory_space_constraint(a, pltpu.VMEM) for a in (attended, log_norm)))


def fused(queries, keys, values, lengths):
    rows, tok, q_width = queries.shape
    kv_width = keys.shape[2]
    heads, shards = lax.axis_size("heads"), lax.axis_size("dp")
    q_heads = q_width // HEAD_SIZE
    dma = pltpu.SemaphoreType.DMA
    results = pl.pallas_call(
        functools.partial(fused_kernel, shards),
        out_shape=(
            pltpu.VMEM((rows, tok, q_width), jnp.bfloat16),
            pltpu.VMEM((q_heads // heads, rows, heads * tok), jnp.float32),
        ),
        in_specs=[pl.BlockSpec(memory_space=pltpu.HBM)] * 4,
        out_specs=(pl.BlockSpec(memory_space=pl.ANY),) * 2,
        scratch_shapes=[
            pltpu.VMEM((rows, 2, 6, tok, kv_width // 2), jnp.bfloat16),
            pltpu.VMEM((rows, 2, tok, q_width // 2), jnp.bfloat16),
            pltpu.VMEM((rows, 2, tok, q_width // 2), jnp.bfloat16),
            pltpu.VMEM(lengths.shape, jnp.int32),
            pltpu.VMEM((rows, 2 * tok, HEAD_SIZE), jnp.int32),
            pltpu.VMEM((2 * tok, HEAD_SIZE), jnp.float32),
            pltpu.VMEM((q_heads // 2, rows, 2 * tok), jnp.float32),
            pltpu.VMEM((rows, q_heads // 2, 2 * tok, 6 * tok), jnp.bfloat16),
            pltpu.VMEM((rows, q_heads // 2, 2 * tok, HEAD_SIZE), jnp.float32),
            pltpu.VMEM((2, tok, kv_width // 2), jnp.bfloat16),
            pltpu.VMEM((2, tok, kv_width // 2), jnp.bfloat16),
            pltpu.VMEM(((shards - 1) // 2, rows // 4, tok, kv_width), jnp.bfloat16),
            pltpu.VMEM(keys.shape, jnp.bfloat16),
            pltpu.VMEM(values.shape, jnp.bfloat16),
            dma, dma, dma, dma((rows, 2)), dma((3 + rows // 2,)), dma, dma, dma, dma((2,)),
            dma(((shards - 1) // 2,)), dma((2,)), pltpu.SemaphoreType.REGULAR,
        ],
        compiler_params=pltpu.CompilerParams(
            collective_id=0, has_side_effects=True, vmem_limit_bytes=48 * 1024 * 1024
        ),
    )(*(pltpu.with_memory_space_constraint(a, pltpu.HBM) for a in (queries, keys, values, lengths)))
    return store(*results)


def dispatch(queries, keys, values, lengths):
    heads, shards = lax.axis_size("heads"), lax.axis_size("dp")
    tok = queries.shape[1]
    suited = (
        heads == 4
        and shards // 8 == 1
        and shards > 2
        and 2 * tok == HEAD_SIZE
        and keys.shape[2] == heads * HEAD_SIZE
        and queries.shape[0] % 2 == 0
        and queries.shape[0] >= 8
        and queries.shape[2] * queries.shape[0] <= 2 * HEAD_SIZE * HEAD_SIZE
    )
    return (fused if suited else per_device)(queries, keys, values, lengths)


def solution(mesh):
    in_specs = (
        P(None, ("dp", "heads"), None),
        P(None, ("dp", "heads"), None),
        P(None, ("dp", "heads"), None),
        P(),
    )
    out_specs = (P(None, ("dp", "heads"), None), P("heads", None, "dp"))
    return jax.shard_map(
        dispatch, mesh=mesh, in_specs=in_specs, out_specs=out_specs, check_vma=False
    )
```
